32 devices in a mesh: seq: 8 (over z, x), tensor: 4 (over y, core).
Axes of the slice: x: 2, y: 2, z: 4, core: 2. Of those that a mesh axis runs over, the one named last changes fastest.
Arguments:
- hidden_in: bfloat16 [16, 5120], replicated, may hold values from -6 to 6
- united_down: bfloat16 [5120, 2112], P(None, 'tensor'), may hold values from -0.078125 to 0.078125
- q_gain: float32 [1536], replicated, may hold values from 0.1 to 1.9
- kv_gain: float32 [512], replicated, may hold values from 0.1 to 1.9
- q_up: bfloat16 [1536, 24576], P('seq', 'tensor'), may hold values from -0.15625 to 0.15625
- key_up: bfloat16 [512, 16384], P(None, 'tensor'), may hold values from -0.25 to 0.25
- value_up: bfloat16 [512, 16384], P(None, 'tensor'), may hold values from -0.0625 to 0.0625
- latent_block_store: bfloat16 [512, 128, 512], P(('seq', 'tensor')), may hold values from -24 to 24
- rope_pool: bfloat16 [512, 64, 128], P(('seq', 'tensor')), may hold values from -124 to 124
- lengths: int32 [16], replicated, may hold values from 2048 to 4096, as said below
- block_table: int32 [16, 32], P(None, 'seq'), may hold values from 0 to 511, as said below
Outputs:
- attn_out: bfloat16 [16, 16384], P(None, 'tensor')
- new_entry: bfloat16 [16, 576], replicated
The draws below stay inside these ranges and needn't reach their ends.
Inputs may be any that keep to these rules, and one draw needn't show every extreme that they name: `lengths`: every sequence holds 2048 to 4096 cached positions; one sequence holds exactly 4096 and another exactly 2048. block_table[b, j] is the pool slot of positions j * 128 to (j + 1) * 128 - 1 of sequence b. The columns j with j // 4 = s name exactly the 64 slots s * 16 * 4 to (s + 1) * 16 * 4 - 1, each once, in any order; blocks past a sequence's length also name such slots.
All inputs are finite; a program needn't handle non-finite values.
Results may differ from the reference program's by a relative error of at most 0.015.
The reference program's roundings to bfloat16 on the way count: a program that leaves them out, or rounds other values in their place, can miss the bound.
Values may be sent and summed in bfloat16 or wider, within the bound.
A program may use at most 128 MiB of HBM per device.

```python
import jax
import jax.numpy as jnp
from jax import lax

D = 5120
QR = 1536
LATENT_RANK = 512
NOPE = 128
ROTARY_WIDTH = 64
VD = 128
H = 128
B = 16
BLOCK_POSITIONS = 128
SPAN_BLK = 4
QH = 192
UNITED = 2112
NBLK = 32
LMAX = 4096
POOL_BLOCKS = 512


def draw_rope_pool(key, part):
    tensor_dims = (POOL_BLOCKS, ROTARY_WIDTH, BLOCK_POSITIONS)
    base_key, active_key, sign_key = jax.random.split(key, 3)
    drawn = jnp.clip(jax.random.normal(base_key, tensor_dims, jnp.float32), -4.0, 4.0)
    return drawn.astype(jnp.bfloat16)


def draw_lengths(key, part):
    first_key, second_key, third_key = jax.random.split(key, 3)
    drawn = jax.random.randint(first_key, (B,), LMAX // 2, LMAX + 1, dtype=jnp.int32)
    longest = jax.random.randint(second_key, (), 0, B, dtype=jnp.int32)
    shortest = (longest + jax.random.randint(third_key, (), 1, B, dtype=jnp.int32)) % B
    seq_ids = jnp.arange(B, dtype=jnp.int32)
    drawn = jnp.where(seq_ids == shortest, LMAX // 2, drawn)
    return jnp.where(seq_ids == longest, LMAX, drawn).astype(jnp.int32)


def draw_block_table(key, part):
    group_size = B * SPAN_BLK
    group_count = NBLK // SPAN_BLK
    group_keys = jax.random.split(key, group_count)
    orders = jax.vmap(lambda one_key: jax.random.permutation(one_key, group_size))(group_keys)
    offsets = jnp.arange(group_count, dtype=jnp.int32)[:, None] * group_size
    placed = (orders.astype(jnp.int32) + offsets).reshape(group_count, B, SPAN_BLK)
    return jnp.transpose(placed, (1, 0, 2)).reshape(B, NBLK).astype(jnp.int32)


def steps_of(rng, dims, pieces, least, high):
    level = 1.0
    for axis_at, blocks in pieces:
        steps = jax.random.uniform(jax.random.fold_in(jax.random.fold_in(rng, 6), axis_at), (blocks,), jnp.float32, least / len(pieces), high / len(pieces))
        level = level * jnp.repeat(jnp.exp(steps), dims[axis_at] // blocks).reshape((-1,) + (1,) * (len(dims) - 1 - axis_at))
    return level


def scatter_about(own_key, dims, spread, limit, cuts=(), kind=jnp.bfloat16):
    array = spread * jax.random.normal(own_key, dims, jnp.float32)
    if cuts:
        array = array * steps_of(own_key, dims, cuts, -0.22, 0.18)
    return jnp.clip(array, -limit, limit).astype(kind)


def setup_inputs(seed: int = 0) -> dict:
    seeds = jax.random.split(jax.random.key(seed), 12)
    hidden_in = scatter_about(seeds[0], (B, D), 1.0, 6.0)
    united_down = scatter_about(seeds[1], (D, UNITED), D ** -0.5, 0.078125, ((1, 4),))
    q_gain = jnp.clip(1.0 + 0.18 * jax.random.normal(seeds[2], (QR,), jnp.float32), 0.1, 1.9)
    kv_gain = jnp.clip(1.0 + 0.18 * jax.random.normal(seeds[3], (LATENT_RANK,), jnp.float32), 0.1, 1.9)
    q_up = scatter_about(seeds[4], (QR, H * QH), QR ** -0.5, 0.15625, ((0, 8), (1, 4)))
    key_up = scatter_about(seeds[5], (LATENT_RANK, H * NOPE), LATENT_RANK ** -0.5, 0.25, ((1, 4),))
    value_up = scatter_about(seeds[6], (LATENT_RANK, H * VD), (16 * LATENT_RANK) ** -0.5, 0.0625, ((1, 4),))
    latent_block_store = scatter_about(seeds[7], (POOL_BLOCKS, BLOCK_POSITIONS, LATENT_RANK), 4.0, 24.0, ((0, 32),))
    rope_pool = draw_rope_pool(jax.random.fold_in(seeds[11], 71), 0)
    lengths = draw_lengths(jax.random.fold_in(seeds[11], 71), 0)
    block_table = draw_block_table(jax.random.fold_in(seeds[11], 71), 0)
    return {"hidden_in": hidden_in, "united_down": united_down, "q_gain": q_gain, "kv_gain": kv_gain, "q_up": q_up, "key_up": key_up, "value_up": value_up, "latent_block_store": latent_block_store, "rope_pool": rope_pool, "lengths": lengths, "block_table": block_table}


NORM_FLOOR = 1.0

def rms_scale(row_values, gain_row):
    mean_square = lax.optimization_barrier(jnp.mean(row_values * row_values, axis=-1, keepdims=True))
    return row_values * lax.rsqrt(mean_square + NORM_FLOOR) * gain_row

def rotate_pairs(rope_pairs, positions):
    half_dim = rope_pairs.shape[-1] // 2
    inverse_freq = 10000.0 ** (-2.0 * jnp.arange(half_dim, dtype=jnp.float32) / rope_pairs.shape[-1])
    angles = positions[..., None] * inverse_freq
    cosine = jnp.cos(angles)
    sine_part = jnp.sin(angles)
    front_half = rope_pairs[..., :half_dim]
    back_half = rope_pairs[..., half_dim:]
    return jnp.concatenate([front_half * cosine - back_half * sine_part, front_half * sine_part + back_half * cosine], axis=-1)

def reference(hidden_in, united_down, q_gain, kv_gain, q_up, key_up, value_up, latent_block_store, rope_pool, lengths, block_table):
    united = jnp.dot(hidden_in, united_down, preferred_element_type=jnp.float32).astype(jnp.bfloat16)
    united_wide = united.astype(jnp.float32)
    positions = lengths.astype(jnp.float32)
    query_latent = rms_scale(united_wide[:, :QR], q_gain).astype(jnp.bfloat16)
    new_latent = rms_scale(united_wide[:, QR:QR + LATENT_RANK], kv_gain).astype(jnp.bfloat16)
    new_rope = rotate_pairs(united_wide[:, QR + LATENT_RANK:], positions).astype(jnp.bfloat16)
    new_entry = jnp.concatenate([new_latent, new_rope], axis=1)
    query_full = jnp.dot(query_latent, q_up, preferred_element_type=jnp.float32).reshape(B, H, QH)
    query_nope = query_full[:, :, :NOPE].astype(jnp.bfloat16)
    key_heads = key_up.reshape(LATENT_RANK, H, NOPE)
    score_scale = QH ** (-0.5)
    absorbed = jnp.einsum('bhn,khn->bhk', query_nope.astype(jnp.float32), key_heads.astype(jnp.float32))
    query_lat = (absorbed * score_scale).astype(jnp.bfloat16)
    query_rot = (rotate_pairs(query_full[:, :, NOPE:], positions[:, None]) * score_scale).astype(jnp.bfloat16)
    cache_rows = jnp.arange(LMAX, dtype=jnp.int32)

    def one_sequence(inputs):
        lat_query, rot_query, table_row, length_one, own_latent, own_rope = inputs
        keys_latent = latent_block_store[table_row].reshape(LMAX, LATENT_RANK)
        keys_rope = jnp.swapaxes(rope_pool[table_row], 1, 2).reshape(LMAX, ROTARY_WIDTH)
        scores = jnp.dot(lat_query, keys_latent.T, preferred_element_type=jnp.float32)
        scores = scores + jnp.dot(rot_query, keys_rope.T, preferred_element_type=jnp.float32)
        valid_mask = cache_rows < length_one
        scores = jnp.where(valid_mask[None, :], scores, -jnp.inf)
        own_score = lax.optimization_barrier(jnp.sum(lat_query.astype(jnp.float32) * own_latent.astype(jnp.float32)[None, :], axis=1))
        own_score = own_score + lax.optimization_barrier(jnp.sum(rot_query.astype(jnp.float32) * own_rope.astype(jnp.float32)[None, :], axis=1))
        top_score = jnp.maximum(lax.optimization_barrier(jnp.max(scores, axis=1)), own_score)
        weights = jnp.exp(scores - top_score[:, None])
        own_weight = jnp.exp(own_score - top_score)
        totals = lax.optimization_barrier(jnp.sum(weights, axis=1)) + own_weight
        mixture = jnp.dot(weights.astype(jnp.bfloat16), keys_latent, preferred_element_type=jnp.float32)
        mixture = mixture + own_weight.astype(jnp.bfloat16).astype(jnp.float32)[:, None] * own_latent.astype(jnp.float32)[None, :]
        return (mixture / totals[:, None]).astype(jnp.bfloat16)
    attended = lax.map(one_sequence, (query_lat, query_rot, block_table, lengths, new_latent, new_rope))
    value_heads = value_up.reshape(LATENT_RANK, H, VD)
    attn_out = jnp.einsum('bhk,khv->bhv', attended.astype(jnp.float32), value_heads.astype(jnp.float32))
    attn_out = attn_out.reshape(B, H * VD).astype(jnp.bfloat16)
    return (attn_out, new_entry)
```

```python
import functools

import jax
import jax.numpy as jnp
from jax import lax
from jax.experimental import pallas as pl
from jax.experimental.pallas import tpu as pltpu
from jax.sharding import PartitionSpec as P

QR = 1536
LATENT_RANK = 512
NOPE = 128
VD = 128
B = 16
BLOCK_POSITIONS = 128
QH = 192


NORM_FLOOR = 1.0
FLOOR_SCORE = -1e30


def rms_scale(row_values, gain_row):
    mean_square = jnp.mean(row_values * row_values, axis=-1, keepdims=True)
    return row_values * lax.rsqrt(mean_square + NORM_FLOOR) * gain_row


def rotate_pairs(rope_pairs, positions):
    half_dim = rope_pairs.shape[-1] // 2
    inverse_freq = 10000.0 ** (
        -2.0 * jnp.arange(half_dim, dtype=jnp.float32) / rope_pairs.shape[-1]
    )
    angles = positions[..., None] * inverse_freq
    cosine = jnp.cos(angles)
    sine_part = jnp.sin(angles)
    front_half = rope_pairs[..., :half_dim]
    back_half = rope_pairs[..., half_dim:]
    return jnp.concatenate(
        [front_half * cosine - back_half * sine_part, front_half * sine_part + back_half * cosine],
        axis=-1,
    )


def attend_slots(query_pack, latent_blocks, rope_blocks, slot_ids, table_flat, base_flat, lengths):
    sequences = query_pack.shape[0]
    span_blocks = table_flat.shape[0] // sequences
    block_rows = latent_blocks.shape[1]
    latent_width = latent_blocks.shape[2]
    flat_index = jnp.arange(table_flat.shape[0], dtype=jnp.int32)
    matches = table_flat[None, :] == slot_ids[:, None]
    owner_seq = jnp.sum(jnp.where(matches, (flat_index // span_blocks)[None, :], 0), axis=1)
    owner_base = jnp.sum(jnp.where(matches, base_flat[None, :], 0), axis=1)
    seq_hot = owner_seq[:, None] == jnp.arange(sequences, dtype=jnp.int32)[None, :]
    picked = jnp.einsum(
        "kb,bhc->khc", seq_hot.astype(jnp.bfloat16), query_pack, preferred_element_type=jnp.float32
    ).astype(jnp.bfloat16)
    scores = jnp.einsum(
        "khc,kpc->khp",
        picked[:, :, :latent_width],
        latent_blocks,
        preferred_element_type=jnp.float32,
    )
    scores = scores + jnp.einsum(
        "khr,krp->khp", picked[:, :, latent_width:], rope_blocks, preferred_element_type=jnp.float32
    )
    limits = jnp.sum(jnp.where(seq_hot, lengths[None, :], 0), axis=1)
    valid_mask = (
        owner_base[:, None] + jnp.arange(block_rows, dtype=jnp.int32)[None, :] < limits[:, None]
    )
    scores = jnp.where(valid_mask[:, None, :], scores, FLOOR_SCORE)
    slot_top = jnp.max(scores, axis=2)
    weights = jnp.where(valid_mask[:, None, :], jnp.exp(scores - slot_top[:, :, None]), 0.0)
    slot_total = jnp.sum(weights, axis=2)
    slot_mixed = jnp.einsum(
        "khp,kpc->khc",
        weights.astype(jnp.bfloat16),
        latent_blocks,
        preferred_element_type=jnp.float32,
    )
    seq_top = jnp.max(jnp.where(seq_hot[:, :, None], slot_top[:, None, :], FLOOR_SCORE), axis=0)
    top_at = jnp.sum(jnp.where(seq_hot[:, :, None], seq_top[None, :, :], 0.0), axis=1)
    factor = jnp.exp(slot_top - top_at)
    hot_wide = seq_hot.astype(jnp.float32)
    seq_total = jnp.einsum(
        "kb,kh->bh", hot_wide, slot_total * factor, precision=lax.Precision.HIGHEST
    )
    seq_mixed = jnp.einsum(
        "kb,khc->bhc", hot_wide, slot_mixed * factor[:, :, None], precision=lax.Precision.HIGHEST
    )
    return (seq_top, seq_total, seq_mixed)


def combine_parts(earlier, later):
    top_one, total_one, mixed_one = earlier
    top_two, total_two, mixed_two = later
    top_both = jnp.maximum(top_one, top_two)
    scale_two = jnp.exp(top_two - top_both)
    return (top_both, total_two * scale_two, mixed_two * scale_two[:, :, None])


def plain_body(
    hidden_in,
    united_down,
    q_gain,
    kv_gain,
    q_up,
    key_up,
    value_up,
    latent_block_store,
    rope_pool,
    lengths,
    block_table,
):
    local_heads = key_up.shape[1] // NOPE
    span_blocks = block_table.shape[1]
    seq_index = lax.axis_index("seq")
    part_cols = jnp.dot(hidden_in, united_down, preferred_element_type=jnp.float32).astype(
        jnp.bfloat16
    )
    united_wide = lax.all_gather(part_cols, "tensor", axis=1, tiled=True).astype(jnp.float32)
    positions = lengths.astype(jnp.float32)
    query_latent = rms_scale(united_wide[:, :QR], q_gain).astype(jnp.bfloat16)
    new_latent = rms_scale(united_wide[:, QR : QR + LATENT_RANK], kv_gain).astype(jnp.bfloat16)
    new_rope = rotate_pairs(united_wide[:, QR + LATENT_RANK :], positions).astype(jnp.bfloat16)
    new_entry = jnp.concatenate([new_latent, new_rope], axis=1)
    row_count = q_up.shape[0]
    own_rows = lax.dynamic_slice_in_dim(query_latent, seq_index * row_count, row_count, 1)
    partial_query = jnp.dot(own_rows, q_up, preferred_element_type=jnp.float32)
    query_full = lax.psum(partial_query, "seq").reshape(B, local_heads, QH)
    query_nope = query_full[:, :, :NOPE].astype(jnp.bfloat16)
    key_heads = key_up.reshape(LATENT_RANK, local_heads, NOPE)
    score_scale = QH ** (-0.5)
    absorbed = jnp.einsum("bhn,khn->bhk", query_nope, key_heads, preferred_element_type=jnp.float32)
    query_lat = (absorbed * score_scale).astype(jnp.bfloat16)
    query_rot = (rotate_pairs(query_full[:, :, NOPE:], positions[:, None]) * score_scale).astype(
        jnp.bfloat16
    )
    query_pack = jnp.concatenate([query_lat, query_rot], axis=2)
    table_flat = block_table.reshape(-1)
    flat_index = jnp.arange(table_flat.shape[0], dtype=jnp.int32)
    base_flat = (seq_index * span_blocks + flat_index % span_blocks) * BLOCK_POSITIONS
    group_base = seq_index * (B * span_blocks)
    initial = (
        jnp.full((B, local_heads), FLOOR_SCORE, jnp.float32),
        jnp.zeros((B, local_heads), jnp.float32),
        jnp.zeros((B, local_heads, LATENT_RANK), jnp.float32),
    )
    latent_piece = lax.all_gather(latent_block_store, "tensor", axis=0, tiled=True)
    rope_piece = lax.all_gather(rope_pool, "tensor", axis=0, tiled=True)
    slot_ids = group_base + jnp.arange(latent_piece.shape[0], dtype=jnp.int32)
    fresh = attend_slots(
        query_pack, latent_piece, rope_piece, slot_ids, table_flat, base_flat, lengths
    )
    top_part, total_part, mixed_part = combine_parts(initial, fresh)
    grand_top = lax.pmax(top_part, "seq")
    factor = jnp.exp(top_part - grand_top)
    total_part, mixed_part = lax.psum((total_part * factor, mixed_part * factor[:, :, None]), "seq")
    top_part = grand_top
    own_score = jnp.sum(
        query_lat.astype(jnp.float32) * new_latent.astype(jnp.float32)[:, None, :], axis=2
    )
    own_score = own_score + jnp.sum(
        query_rot.astype(jnp.float32) * new_rope.astype(jnp.float32)[:, None, :], axis=2
    )
    final_top = jnp.maximum(top_part, own_score)
    old_scale = jnp.exp(top_part - final_top)
    own_weight = jnp.exp(own_score - final_top)
    totals = total_part * old_scale + own_weight
    mixture = mixed_part * old_scale[:, :, None]
    mixture = (
        mixture
        + own_weight.astype(jnp.bfloat16).astype(jnp.float32)[:, :, None]
        * new_latent.astype(jnp.float32)[:, None, :]
    )
    attended = (mixture / totals[:, :, None]).astype(jnp.bfloat16)
    value_heads = value_up.reshape(LATENT_RANK, local_heads, VD)
    attn_out = jnp.einsum("bhk,khv->bhv", attended, value_heads, preferred_element_type=jnp.float32)
    attn_out = attn_out.reshape(B, local_heads * VD).astype(jnp.bfloat16)
    return (attn_out, new_entry)


MESH_ID = pl.DeviceIdType.MESH
LANES = 128
UNITED_CHUNKS = 5
GROUP = 4


def split_three(value):
    high = value.astype(jnp.bfloat16)
    rest = value - high.astype(jnp.float32)
    middle = rest.astype(jnp.bfloat16)
    low = (rest - middle.astype(jnp.float32)).astype(jnp.bfloat16)
    return high, middle, low


def rotate_wide(wide, cos_wide, sin_wide, lane_at, half):
    partner = jnp.where(
        lane_at < half, pltpu.roll(wide, LANES - half, 1), pltpu.roll(wide, half, 1)
    )
    return wide * cos_wide + partner * sin_wide


def step_kernel(
    n_seq,
    n_tensor,
    dims,
    idx_ref,
    len_ref,
    hidden_ref,
    cos_ref,
    sin_ref,
    q_gain_ref,
    kv_gain_ref,
    ud_hbm,
    qu_hbm,
    ku_hbm,
    vu_hbm,
    lat_hbm,
    rope_hbm,
    out_ref,
    ne_ref,
    ud_vm,
    qu_vm,
    ku_vm,
    vu_vm,
    lat_vm,
    rope_vm,
    uni_vm,
    uw_vm,
    ql_vm,
    nep_vm,
    qs_vm,
    qr_vm,
    pack_vm,
    qall_vm,
    mix_vm,
    top_vm,
    tot_vm,
    mixall_vm,
    part_vm,
    got_vm,
    out_vm,
    ud_sem,
    w_sem,
    loc_sem,
    u_send,
    u_recv,
    y_send,
    y_recv,
    c_send,
    c_recv,
    d_send,
    d_recv,
    q_send,
    q_recv,
    p_send,
    p_recv,
    m_send,
    m_recv,
    o_send,
    o_recv,
):
    heads = dims["heads"]
    own_heads = dims["own_heads"]
    batch = dims["batch"]
    span_blocks = dims["span_blocks"]
    blocks = dims["blocks"]
    united_cols = dims["united_cols"]
    rope_width = dims["rope_width"]
    rows = dims["rows"]
    rank = LATENT_RANK
    pack_width = rank + LANES
    own_rows = own_heads * batch
    all_rows = heads * batch
    groups = blocks // GROUP
    s = lax.axis_index("seq")
    t = lax.axis_index("tensor")
    core_mate = t + 1 - 2 * (t % 2)
    far_mate = (t + 2) % n_tensor
    diagonal = (core_mate + 2) % n_tensor

    def at_seq(i):
        return {"seq": (s + i) % n_seq}

    depth = hidden_ref.shape[1] // UNITED_CHUNKS
    ud_copies = [
        pltpu.make_async_copy(
            ud_hbm.at[pl.ds(i * depth, depth)], ud_vm.at[pl.ds(i * depth, depth)], ud_sem.at[i]
        )
        for i in range(UNITED_CHUNKS)
    ]
    for copy in ud_copies:
        copy.start()
    head_cols = pl.ds(pl.multiple_of(s * (own_heads * NOPE), LANES), own_heads * NOPE)
    qu_copy = pltpu.make_async_copy(qu_hbm, qu_vm, w_sem.at[0])
    ku_copy = pltpu.make_async_copy(ku_hbm.at[:, head_cols], ku_vm, w_sem.at[1])
    vu_copy = pltpu.make_async_copy(vu_hbm.at[:, head_cols], vu_vm, w_sem.at[2])
    lat_copy = pltpu.make_async_copy(lat_hbm, lat_vm.at[t], loc_sem.at[0])
    rope_copy = pltpu.make_async_copy(rope_hbm, rope_vm.at[t], loc_sem.at[1])
    for copy in (qu_copy, ku_copy, vu_copy, lat_copy, rope_copy):
        copy.start()

    barrier = pltpu.get_barrier_semaphore()
    for i in range(1, n_seq):
        pl.semaphore_signal(barrier, inc=1, device_id=at_seq(i), device_id_type=MESH_ID)
    for i in range(1, n_tensor):
        pl.semaphore_signal(
            barrier, inc=1, device_id={"tensor": (t + i) % n_tensor}, device_id_type=MESH_ID
        )
    pl.semaphore_wait(barrier, n_seq - 1 + n_tensor - 1)

    def block_copies(src_lat, src_rope, owner, c, send, recv, target):
        at = pl.ds(c * GROUP, GROUP)
        return (
            pltpu.make_async_remote_copy(
                src_ref=src_lat.at[at],
                dst_ref=lat_vm.at[owner, at],
                send_sem=send.at[c, 0],
                recv_sem=recv.at[c, 0],
                device_id={"tensor": target},
                device_id_type=MESH_ID,
            ),
            pltpu.make_async_remote_copy(
                src_ref=src_rope.at[at],
                dst_ref=rope_vm.at[owner, at],
                send_sem=send.at[c, 1],
                recv_sem=recv.at[c, 1],
                device_id={"tensor": target},
                device_id_type=MESH_ID,
            ),
        )

    def y_copies(c):
        return block_copies(lat_hbm, rope_hbm, t, c, y_send, y_recv, far_mate)

    def c_copies(c):
        return block_copies(lat_hbm, rope_hbm, t, c, c_send, c_recv, core_mate)

    def d_copies(c):
        return block_copies(
            lat_vm.at[far_mate], rope_vm.at[far_mate], far_mate, c, d_send, d_recv, core_mate
        )

    total = jnp.zeros((batch, united_cols), jnp.float32)
    for i, copy in enumerate(ud_copies):
        copy.wait()
        total = total + jnp.dot(
            hidden_ref[:, i * depth : (i + 1) * depth],
            ud_vm[i * depth : (i + 1) * depth, :],
            preferred_element_type=jnp.float32,
        )
    uni_vm[t] = jnp.zeros(uni_vm.shape[1:], jnp.bfloat16)
    uni_vm[t, :, :united_cols] = total.astype(jnp.bfloat16)

    def u_copy(i):
        return pltpu.make_async_remote_copy(
            src_ref=uni_vm.at[t],
            dst_ref=uni_vm.at[t],
            send_sem=u_send.at[i],
            recv_sem=u_recv.at[i],
            device_id={"tensor": (t + i) % n_tensor},
            device_id_type=MESH_ID,
        )

    u_copies = [u_copy(i) for i in range(1, n_tensor)]
    for copy in u_copies:
        copy.start()
    for c in range(groups):
        for copy in y_copies(c):
            copy.start()
    for c in range(groups):
        for copy in c_copies(c):
            copy.start()
    for copy in u_copies:
        copy.wait()
    uw_vm[...] = jnp.zeros(uw_vm.shape, jnp.float32)
    wide_cols = uni_vm.shape[2]
    for i in range(n_tensor):
        base = united_cols * i // LANES * LANES
        shift = united_cols * i - base
        piece = uni_vm[i].astype(jnp.float32)
        if shift:
            piece = pltpu.roll(piece, shift, 1)
        uw_vm[:, base : base + wide_cols] = uw_vm[:, base : base + wide_cols] + piece

    lane_at = lax.broadcasted_iota(jnp.int32, (batch, LANES), 1)
    half = rope_width // 2
    cos_wide = cos_ref[...]
    sin_wide = sin_ref[...]
    latent_part = uw_vm[:, :QR]
    ql_vm[...] = rms_scale(latent_part, q_gain_ref[...]).astype(jnp.bfloat16).astype(jnp.float32)
    new_latent = rms_scale(uw_vm[:, QR : QR + rank], kv_gain_ref[...]).astype(jnp.bfloat16)
    new_rope = rotate_wide(
        uw_vm[:, QR + rank : QR + rank + LANES], cos_wide, sin_wide, lane_at, half
    ).astype(jnp.bfloat16)
    ne_ref[:, :rank] = new_latent
    ne_ref[:, rank:] = new_rope[:, :rope_width]
    nep_vm[:, :rank] = new_latent.astype(jnp.float32)
    nep_vm[:, rank:] = new_rope.astype(jnp.float32)

    row_base = pl.multiple_of(s * rows // LANES * LANES, LANES)
    row_window = ql_vm[:, pl.ds(row_base, 2 * LANES)]
    row_window = jnp.where(
        (s * rows) % LANES == 0, row_window, pltpu.roll(row_window, 2 * LANES - LANES // 2, 1)
    )
    own_query = row_window[:, :rows].astype(jnp.bfloat16)
    qu_copy.wait()
    chunk_cols = own_heads * QH

    def q_copy(i):
        return pltpu.make_async_remote_copy(
            src_ref=qs_vm.at[i],
            dst_ref=qr_vm.at[i],
            send_sem=q_send.at[i],
            recv_sem=q_recv.at[i],
            device_id=at_seq(i),
            device_id_type=MESH_ID,
        )

    for i in list(range(1, n_seq)) + [0]:
        cols = pl.ds(pl.multiple_of((s + i) % n_seq * chunk_cols, LANES), chunk_cols)
        qs_vm[i] = jnp.dot(own_query, qu_vm[:, cols], preferred_element_type=jnp.float32)
        if i:
            q_copy(i).start()
    query = qs_vm[0]
    for i in range(1, n_seq):
        q_copy(i).wait()
        query = query + qr_vm[i]

    score_scale = QH ** (-0.5)
    ku_copy.wait()
    pair = 2 * QH
    for h in range(own_heads):
        both = query[:, h // 2 * pair : (h // 2 + 1) * pair]
        start = 0
        if h % 2:
            both = pltpu.roll(both, pair - LANES // 2, 1)
            start = LANES
        nope = both[:, start : start + NOPE].astype(jnp.bfloat16)
        if h % 2:
            rope = both[:, 2 * LANES : 3 * LANES]
        else:
            rope = both[:, LANES : 2 * LANES]
        absorbed = lax.dot_general(
            nope,
            ku_vm[:, h * NOPE : (h + 1) * NOPE],
            (((1,), (1,)), ((), ())),
            preferred_element_type=jnp.float32,
        )
        at = pl.ds(h * batch, batch)
        pack_vm[0, at, :rank] = (absorbed * score_scale).astype(jnp.bfloat16)
        pack_vm[0, at, rank:] = (
            rotate_wide(rope, cos_wide, sin_wide, lane_at, half) * score_scale
        ).astype(jnp.bfloat16)

    def p_copy(i):
        return pltpu.make_async_remote_copy(
            src_ref=pack_vm.at[0],
            dst_ref=pack_vm.at[i],
            send_sem=p_send.at[i],
            recv_sem=p_recv.at[i],
            device_id=at_seq(i),
            device_id_type=MESH_ID,
        )

    for i in range(1, n_seq):
        p_copy(i).start()
    for i in range(1, n_seq):
        p_copy(i).wait()
    for b0 in range(0, batch, 4):
        part_rows = 4 * heads
        want = lax.broadcasted_iota(jnp.int32, (part_rows, all_rows), 0)
        have = lax.broadcasted_iota(jnp.int32, (part_rows, all_rows), 1)
        want_b = b0 + want // heads
        want_h = want % heads
        slot = (s + n_seq - want_h // own_heads) % n_seq
        source = slot * own_rows + want_h % own_heads * batch + want_b
        hot = jnp.where(have == source, 1.0, 0.0).astype(jnp.bfloat16)
        ordered = jnp.dot(
            hot,
            pack_vm[...].reshape(all_rows, pack_width),
            preferred_element_type=jnp.float32,
        ).astype(jnp.bfloat16)
        qall_vm[b0 : b0 + 4] = ordered.reshape(4, heads, pack_width)

    position = lax.broadcasted_iota(jnp.int32, (heads, BLOCK_POSITIONS), 1)

    def attend_one(owner, k):
        slot = owner * blocks + k
        flat = idx_ref[slot]
        seq_of = flat // span_blocks
        base = (s * span_blocks + flat % span_blocks) * BLOCK_POSITIONS
        limit = len_ref[seq_of] - base
        q = qall_vm[seq_of]
        latent = lat_vm[owner, k]
        scores = lax.dot_general(
            q[:, :rank], latent, (((1,), (1,)), ((), ())), preferred_element_type=jnp.float32
        )
        scores = scores + jnp.dot(
            q[:, rank : rank + rope_width], rope_vm[owner, k], preferred_element_type=jnp.float32
        )
        valid = position < limit
        scores = jnp.where(valid, scores, FLOOR_SCORE)
        top = jnp.max(scores, axis=1, keepdims=True)
        weights = jnp.where(valid, jnp.exp(scores - top), 0.0)
        amount = jnp.sum(weights, axis=1, keepdims=True)
        mixed = jnp.dot(weights.astype(jnp.bfloat16), latent, preferred_element_type=jnp.float32)
        mix_vm[slot] = mixed
        top_vm[slot] = jnp.broadcast_to(top, (heads, LANES))
        tot_vm[slot] = jnp.broadcast_to(amount, (heads, LANES))

    def attend_group(owner, c):
        for k in range(GROUP):
            attend_one(owner, c * GROUP + k)

    lat_copy.wait()
    rope_copy.wait()

    def own_step(c, carry):
        attend_group(t, c)
        return carry

    lax.fori_loop(0, groups, own_step, 0)

    def mate_step(c, carry):
        for copy in c_copies(c):
            copy.wait()
        attend_group(core_mate, c)
        return carry

    lax.fori_loop(0, groups, mate_step, 0)

    def far_step(c, carry):
        for copy in y_copies(c):
            copy.wait()
        for copy in d_copies(c):
            copy.start()
        attend_group(far_mate, c)
        for copy in d_copies(c):
            copy.wait()
        attend_group(diagonal, c)
        return carry

    lax.fori_loop(0, groups, far_step, 0)

    lane_wide = lax.broadcasted_iota(jnp.int32, (heads, LANES), 1)

    def merge_step(b, carry):
        slots = [idx_ref[n_tensor * blocks + b * span_blocks + j] for j in range(span_blocks)]
        tops = [top_vm[slot] for slot in slots]
        top = functools.reduce(jnp.maximum, tops)
        total = jnp.zeros((heads, LANES), jnp.float32)
        mixed = jnp.zeros((heads, rank), jnp.float32)
        for slot, one in zip(slots, tops):
            factor = jnp.exp(one - top)
            total = total + tot_vm[slot] * factor
            mixed = mixed + mix_vm[slot] * factor[:, :1]
        stats = jnp.zeros((heads, LANES), jnp.float32)
        for lane, piece in enumerate(split_three(top) + split_three(total)):
            stats = jnp.where(lane_wide == lane, piece.astype(jnp.float32), stats)
        at = pl.ds(pl.multiple_of(b * heads, heads), heads)
        mixall_vm[at, :rank] = mixed.astype(jnp.bfloat16)
        mixall_vm[at, rank:] = stats.astype(jnp.bfloat16)
        return carry

    lax.fori_loop(0, batch, merge_step, 0)

    def m_copy(i):
        return pltpu.make_async_remote_copy(
            src_ref=part_vm.at[i],
            dst_ref=got_vm.at[i],
            send_sem=m_send.at[i],
            recv_sem=m_recv.at[i],
            device_id=at_seq(i),
            device_id_type=MESH_ID,
        )

    want = lax.broadcasted_iota(jnp.int32, (own_rows, all_rows), 0)
    have = lax.broadcasted_iota(jnp.int32, (own_rows, all_rows), 1)
    local_source = want % batch * heads + want // batch
    for i in list(range(1, n_seq)) + [0]:
        peer = (s + i) % n_seq
        hot = jnp.where(have == local_source + peer * own_heads, 1.0, 0.0).astype(jnp.bfloat16)
        chosen = jnp.dot(hot, mixall_vm[...], preferred_element_type=jnp.float32).astype(
            jnp.bfloat16
        )
        if i:
            part_vm[i] = chosen
            m_copy(i).start()
        else:
            got_vm[0] = chosen

    pack = pack_vm[0].astype(jnp.float32)
    entry = jnp.concatenate([nep_vm[...]] * own_heads, axis=0)
    own_score = jnp.sum(pack * entry, axis=1, keepdims=True)
    for i in range(1, n_seq):
        m_copy(i).wait()
    tops = []
    totals = []
    for i in range(n_seq):
        stats = got_vm[i, :, rank:].astype(jnp.float32)
        tops.append(stats[:, 0:1] + stats[:, 1:2] + stats[:, 2:3])
        totals.append(stats[:, 3:4] + stats[:, 4:5] + stats[:, 5:6])
    final_top = functools.reduce(jnp.maximum, tops, own_score)
    own_weight = jnp.exp(own_score - final_top)
    total = own_weight
    mixture = own_weight.astype(jnp.bfloat16).astype(jnp.float32) * entry[:, :rank]
    for i in range(n_seq):
        factor = jnp.exp(tops[i] - final_top)
        total = total + totals[i] * factor
        mixture = mixture + got_vm[i, :, :rank].astype(jnp.float32) * factor
    attended = (mixture / total).astype(jnp.bfloat16)
    vu_copy.wait()
    for h in range(own_heads):
        out_vm[0, :, h * VD : (h + 1) * VD] = jnp.dot(
            attended[h * batch : (h + 1) * batch],
            vu_vm[:, h * VD : (h + 1) * VD],
            preferred_element_type=jnp.float32,
        ).astype(jnp.bfloat16)

    def o_copy(i):
        return pltpu.make_async_remote_copy(
            src_ref=out_vm.at[0],
            dst_ref=out_vm.at[i],
            send_sem=o_send.at[i],
            recv_sem=o_recv.at[i],
            device_id=at_seq(i),
            device_id_type=MESH_ID,
        )

    for i in range(1, n_seq):
        o_copy(i).start()
    for i in range(n_seq):
        if i:
            o_copy(i).wait()
        cols = pl.ds(
            pl.multiple_of((s + n_seq - i) % n_seq * (own_heads * VD), LANES), own_heads * VD
        )
        out_ref[:, cols] = out_vm[i]


def kernel_body(
    n_seq,
    n_tensor,
    hidden_in,
    united_down,
    q_gain,
    kv_gain,
    q_up,
    key_up,
    value_up,
    latent_block_store,
    rope_pool,
    lengths,
    block_table,
):
    batch, width = hidden_in.shape
    heads = key_up.shape[1] // NOPE
    own_heads = heads // n_seq
    span_blocks = block_table.shape[1]
    blocks = latent_block_store.shape[0]
    rope_width = rope_pool.shape[1]
    united_cols = united_down.shape[1]
    seq_index = lax.axis_index("seq")
    local_table = block_table.reshape(-1) - seq_index * (batch * span_blocks)
    flat_index = jnp.arange(local_table.shape[0], dtype=jnp.int32)
    slot_at = jnp.arange(n_tensor * blocks, dtype=jnp.int32)
    owner = jnp.sum(
        jnp.where(local_table[None, :] == slot_at[:, None], flat_index[None, :], 0), axis=1
    )
    places = jnp.concatenate([owner, local_table])
    half = rope_width // 2
    lane = jnp.arange(LANES, dtype=jnp.int32)
    freq = 10000.0 ** (-2.0 * (lane % half).astype(jnp.float32) / rope_width)
    angles = lengths.astype(jnp.float32)[:, None] * freq[None, :]
    inside = (lane < rope_width)[None, :]
    cos_wide = jnp.where(inside, jnp.cos(angles), 0.0)
    sine = jnp.sin(angles)
    sin_wide = jnp.where(inside, jnp.where((lane < half)[None, :], -sine, sine), 0.0)
    dims = dict(
        heads=heads,
        own_heads=own_heads,
        batch=batch,
        span_blocks=span_blocks,
        blocks=blocks,
        united_cols=united_cols,
        rope_width=rope_width,
        rows=q_up.shape[0],
    )
    wide_cols = -(-united_cols // LANES) * LANES
    united_all = -(-united_cols * n_tensor // LANES) * LANES + 4 * LANES
    pack_width = LATENT_RANK + LANES
    own_rows = own_heads * batch
    all_rows = heads * batch
    groups = blocks // GROUP
    slots = n_tensor * blocks
    vmem = pl.BlockSpec(memory_space=pltpu.VMEM)
    smem = pl.BlockSpec(memory_space=pltpu.SMEM)
    anywhere = pl.BlockSpec(memory_space=pl.ANY)
    dma = pltpu.SemaphoreType.DMA
    bf16, f32 = jnp.bfloat16, jnp.float32
    out, new_entry = pl.pallas_call(
        functools.partial(step_kernel, n_seq, n_tensor, dims),
        out_shape=(
            jax.ShapeDtypeStruct((batch, heads * VD), bf16),
            jax.ShapeDtypeStruct((batch, LATENT_RANK + rope_width), bf16),
        ),
        in_specs=[smem, smem] + [vmem] * 5 + [anywhere] * 6,
        out_specs=(vmem, vmem),
        scratch_shapes=[
            pltpu.VMEM(united_down.shape, bf16),
            pltpu.VMEM(q_up.shape, bf16),
            pltpu.VMEM((LATENT_RANK, own_heads * NOPE), bf16),
            pltpu.VMEM((LATENT_RANK, own_heads * VD), bf16),
            pltpu.VMEM((n_tensor,) + latent_block_store.shape, bf16),
            pltpu.VMEM((n_tensor,) + rope_pool.shape, bf16),
            pltpu.VMEM((n_tensor, batch, wide_cols), bf16),
            pltpu.VMEM((batch, united_all), f32),
            pltpu.VMEM((batch, QR), f32),
            pltpu.VMEM((batch, pack_width), f32),
            pltpu.VMEM((n_seq, batch, own_heads * QH), f32),
            pltpu.VMEM((n_seq, batch, own_heads * QH), f32),
            pltpu.VMEM((n_seq, own_rows, pack_width), bf16),
            pltpu.VMEM((batch, heads, pack_width), bf16),
            pltpu.VMEM((slots, heads, LATENT_RANK), f32),
            pltpu.VMEM((slots, heads, LANES), f32),
            pltpu.VMEM((slots, heads, LANES), f32),
            pltpu.VMEM((all_rows, pack_width), bf16),
            pltpu.VMEM((n_seq, own_rows, pack_width), bf16),
            pltpu.VMEM((n_seq, own_rows, pack_width), bf16),
            pltpu.VMEM((n_seq, batch, own_heads * VD), bf16),
            dma((UNITED_CHUNKS,)),
            dma((3,)),
            dma((2,)),
            dma((n_tensor,)),
            dma((n_tensor,)),
            dma((groups, 2)),
            dma((groups, 2)),
            dma((groups, 2)),
            dma((groups, 2)),
            dma((groups, 2)),
            dma((groups, 2)),
        ]
        + [dma((n_seq,))] * 8,
        compiler_params=pltpu.CompilerParams(
            collective_id=0, has_side_effects=True, vmem_limit_bytes=60 * 1024 * 1024
        ),
    )(
        places,
        lengths,
        hidden_in,
        cos_wide,
        sin_wide,
        q_gain[None, :],
        kv_gain[None, :],
        united_down,
        q_up,
        key_up,
        value_up,
        latent_block_store,
        rope_pool,
    )
    return (out, new_entry)


def body_for(n_seq, n_tensor):
    def body(*args):
        q_up, key_up, latents = args[4], args[5], args[7]
        heads = key_up.shape[1] // NOPE
        fits = n_tensor == 4 and heads % (2 * n_seq) == 0 and latents.shape[0] % GROUP == 0
        fits = fits and q_up.shape[0] % (LANES // 2) == 0 and q_up.shape[0] <= LANES + LANES // 2
        if fits:
            return kernel_body(n_seq, n_tensor, *args)
        return plain_body(*args)

    return body


def solution(mesh):
    in_specs = (
        P(),
        P(None, "tensor"),
        P(),
        P(),
        P("seq", "tensor"),
        P(None, "tensor"),
        P(None, "tensor"),
        P(("seq", "tensor"), None, None),
        P(("seq", "tensor"), None, None),
        P(),
        P(None, "seq"),
    )
    out_specs = (P(None, "tensor"), P())
    return jax.shard_map(
        body_for(mesh.shape["seq"], mesh.shape["tensor"]), mesh=mesh, in_specs=in_specs, out_specs=out_specs, check_vma=False)
```

```python
import functools
import math

import jax
import jax.numpy as jnp
from jax import lax
from jax.experimental import pallas as pl
from jax.experimental.pallas import tpu as pltpu
from jax.sharding import PartitionSpec as P

QR = 1536
LATENT_RANK = 512
NOPE = 128
VD = 128
B = 16
BLOCK_POSITIONS = 128
QH = 192


NORM_FLOOR = 1.0
FLOOR_SCORE = -1e30


def rms_scale(row_values, gain_row):
    mean_square = jnp.mean(row_values * row_values, axis=-1, keepdims=True)
    return row_values * lax.rsqrt(mean_square + NORM_FLOOR) * gain_row


def rotate_pairs(rope_pairs, positions):
    half_dim = rope_pairs.shape[-1] // 2
    inverse_freq = 10000.0 ** (
        -2.0 * jnp.arange(half_dim, dtype=jnp.float32) / rope_pairs.shape[-1]
    )
    angles = positions[..., None] * inverse_freq
    cosine = jnp.cos(angles)
    sine_part = jnp.sin(angles)
    front_half = rope_pairs[..., :half_dim]
    back_half = rope_pairs[..., half_dim:]
    return jnp.concatenate(
        [front_half * cosine - back_half * sine_part, front_half * sine_part + back_half * cosine],
        axis=-1,
    )


def attend_slots(query_pack, latent_blocks, rope_blocks, slot_ids, table_flat, base_flat, lengths):
    sequences = query_pack.shape[0]
    span_blocks = table_flat.shape[0] // sequences
    block_rows = latent_blocks.shape[1]
    latent_width = latent_blocks.shape[2]
    flat_index = jnp.arange(table_flat.shape[0], dtype=jnp.int32)
    matches = table_flat[None, :] == slot_ids[:, None]
    owner_seq = jnp.sum(jnp.where(matches, (flat_index // span_blocks)[None, :], 0), axis=1)
    owner_base = jnp.sum(jnp.where(matches, base_flat[None, :], 0), axis=1)
    seq_hot = owner_seq[:, None] == jnp.arange(sequences, dtype=jnp.int32)[None, :]
    picked = jnp.einsum(
        "kb,bhc->khc", seq_hot.astype(jnp.bfloat16), query_pack, preferred_element_type=jnp.float32
    ).astype(jnp.bfloat16)
    scores = jnp.einsum(
        "khc,kpc->khp",
        picked[:, :, :latent_width],
        latent_blocks,
        preferred_element_type=jnp.float32,
    )
    scores = scores + jnp.einsum(
        "khr,krp->khp", picked[:, :, latent_width:], rope_blocks, preferred_element_type=jnp.float32
    )
    limits = jnp.sum(jnp.where(seq_hot, lengths[None, :], 0), axis=1)
    valid_mask = (
        owner_base[:, None] + jnp.arange(block_rows, dtype=jnp.int32)[None, :] < limits[:, None]
    )
    scores = jnp.where(valid_mask[:, None, :], scores, FLOOR_SCORE)
    slot_top = jnp.max(scores, axis=2)
    weights = jnp.where(valid_mask[:, None, :], jnp.exp(scores - slot_top[:, :, None]), 0.0)
    slot_total = jnp.sum(weights, axis=2)
    slot_mixed = jnp.einsum(
        "khp,kpc->khc",
        weights.astype(jnp.bfloat16),
        latent_blocks,
        preferred_element_type=jnp.float32,
    )
    seq_top = jnp.max(jnp.where(seq_hot[:, :, None], slot_top[:, None, :], FLOOR_SCORE), axis=0)
    top_at = jnp.sum(jnp.where(seq_hot[:, :, None], seq_top[None, :, :], 0.0), axis=1)
    factor = jnp.exp(slot_top - top_at)
    hot_wide = seq_hot.astype(jnp.float32)
    seq_total = jnp.einsum(
        "kb,kh->bh", hot_wide, slot_total * factor, precision=lax.Precision.HIGHEST
    )
    seq_mixed = jnp.einsum(
        "kb,khc->bhc", hot_wide, slot_mixed * factor[:, :, None], precision=lax.Precision.HIGHEST
    )
    return (seq_top, seq_total, seq_mixed)


def combine_parts(earlier, later):
    top_one, total_one, mixed_one = earlier
    top_two, total_two, mixed_two = later
    top_both = jnp.maximum(top_one, top_two)
    scale_two = jnp.exp(top_two - top_both)
    return (top_both, total_two * scale_two, mixed_two * scale_two[:, :, None])


def plain_body(
    hidden_in,
    united_down,
    q_gain,
    kv_gain,
    q_up,
    key_up,
    value_up,
    latent_block_store,
    rope_pool,
    lengths,
    block_table,
):
    local_heads = key_up.shape[1] // NOPE
    span_blocks = block_table.shape[1]
    seq_index = lax.axis_index("seq")
    part_cols = jnp.dot(hidden_in, united_down, preferred_element_type=jnp.float32).astype(
        jnp.bfloat16
    )
    united_wide = lax.all_gather(part_cols, "tensor", axis=1, tiled=True).astype(jnp.float32)
    positions = lengths.astype(jnp.float32)
    query_latent = rms_scale(united_wide[:, :QR], q_gain).astype(jnp.bfloat16)
    new_latent = rms_scale(united_wide[:, QR : QR + LATENT_RANK], kv_gain).astype(jnp.bfloat16)
    new_rope = rotate_pairs(united_wide[:, QR + LATENT_RANK :], positions).astype(jnp.bfloat16)
    new_entry = jnp.concatenate([new_latent, new_rope], axis=1)
    row_count = q_up.shape[0]
    own_rows = lax.dynamic_slice_in_dim(query_latent, seq_index * row_count, row_count, 1)
    partial_query = jnp.dot(own_rows, q_up, preferred_element_type=jnp.float32)
    query_full = lax.psum(partial_query, "seq").reshape(B, local_heads, QH)
    query_nope = query_full[:, :, :NOPE].astype(jnp.bfloat16)
    key_heads = key_up.reshape(LATENT_RANK, local_heads, NOPE)
    score_scale = QH ** (-0.5)
    absorbed = jnp.einsum("bhn,khn->bhk", query_nope, key_heads, preferred_element_type=jnp.float32)
    query_lat = (absorbed * score_scale).astype(jnp.bfloat16)
    query_rot = (rotate_pairs(query_full[:, :, NOPE:], positions[:, None]) * score_scale).astype(
        jnp.bfloat16
    )
    query_pack = jnp.concatenate([query_lat, query_rot], axis=2)
    table_flat = block_table.reshape(-1)
    flat_index = jnp.arange(table_flat.shape[0], dtype=jnp.int32)
    base_flat = (seq_index * span_blocks + flat_index % span_blocks) * BLOCK_POSITIONS
    group_base = seq_index * (B * span_blocks)
    initial = (
        jnp.full((B, local_heads), FLOOR_SCORE, jnp.float32),
        jnp.zeros((B, local_heads), jnp.float32),
        jnp.zeros((B, local_heads, LATENT_RANK), jnp.float32),
    )
    latent_piece = lax.all_gather(latent_block_store, "tensor", axis=0, tiled=True)
    rope_piece = lax.all_gather(rope_pool, "tensor", axis=0, tiled=True)
    slot_ids = group_base + jnp.arange(latent_piece.shape[0], dtype=jnp.int32)
    fresh = attend_slots(
        query_pack, latent_piece, rope_piece, slot_ids, table_flat, base_flat, lengths
    )
    top_part, total_part, mixed_part = combine_parts(initial, fresh)
    grand_top = lax.pmax(top_part, "seq")
    factor = jnp.exp(top_part - grand_top)
    total_part, mixed_part = lax.psum((total_part * factor, mixed_part * factor[:, :, None]), "seq")
    top_part = grand_top
    own_score = jnp.sum(
        query_lat.astype(jnp.float32) * new_latent.astype(jnp.float32)[:, None, :], axis=2
    )
    own_score = own_score + jnp.sum(
        query_rot.astype(jnp.float32) * new_rope.astype(jnp.float32)[:, None, :], axis=2
    )
    final_top = jnp.maximum(top_part, own_score)
    old_scale = jnp.exp(top_part - final_top)
    own_weight = jnp.exp(own_score - final_top)
    totals = total_part * old_scale + own_weight
    mixture = mixed_part * old_scale[:, :, None]
    mixture = (
        mixture
        + own_weight.astype(jnp.bfloat16).astype(jnp.float32)[:, :, None]
        * new_latent.astype(jnp.float32)[:, None, :]
    )
    attended = (mixture / totals[:, :, None]).astype(jnp.bfloat16)
    value_heads = value_up.reshape(LATENT_RANK, local_heads, VD)
    attn_out = jnp.einsum("bhk,khv->bhv", attended, value_heads, preferred_element_type=jnp.float32)
    attn_out = attn_out.reshape(B, local_heads * VD).astype(jnp.bfloat16)
    return (attn_out, new_entry)


MESH_ID = pl.DeviceIdType.MESH
LANES = 128
UNITED_CHUNKS = 5
GROUP = 4


def split_three(value):
    high = value.astype(jnp.bfloat16)
    rest = value - high.astype(jnp.float32)
    middle = rest.astype(jnp.bfloat16)
    low = (rest - middle.astype(jnp.float32)).astype(jnp.bfloat16)
    return high, middle, low


def rotate_wide(wide, cos_wide, sin_wide, lane_at, half):
    partner = jnp.where(
        lane_at < half, pltpu.roll(wide, LANES - half, 1), pltpu.roll(wide, half, 1)
    )
    return wide * cos_wide + partner * sin_wide


def step_kernel(
    n_seq,
    n_tensor,
    dims,
    idx_ref,
    len_ref,
    hidden_ref,
    q_gain_ref,
    kv_gain_ref,
    ud_hbm,
    qu_hbm,
    ku_hbm,
    vu_hbm,
    lat_hbm,
    rope_hbm,
    out_ref,
    ne_ref,
    ud_vm,
    qu_vm,
    ku_vm,
    vu_vm,
    lat_vm,
    rope_vm,
    uni_vm,
    uw_vm,
    ql_vm,
    nep_vm,
    qs_vm,
    qr_vm,
    pack_vm,
    qall_vm,
    mix_vm,
    top_vm,
    tot_vm,
    mixall_vm,
    part_vm,
    got_vm,
    out_vm,
    ud_sem,
    w_sem,
    loc_sem,
    u_send,
    u_recv,
    y_send,
    y_recv,
    c_send,
    c_recv,
    d_send,
    d_recv,
    q_send,
    q_recv,
    p_send,
    p_recv,
    m_send,
    m_recv,
    o_send,
    o_recv,
):
    heads = dims["heads"]
    own_heads = dims["own_heads"]
    batch = dims["batch"]
    span_blocks = dims["span_blocks"]
    blocks = dims["blocks"]
    united_cols = dims["united_cols"]
    rope_width = dims["rope_width"]
    rows = dims["rows"]
    rank = LATENT_RANK
    pack_width = rank + LANES
    own_rows = own_heads * batch
    all_rows = heads * batch
    groups = blocks // GROUP
    s = lax.axis_index("seq")
    t = lax.axis_index("tensor")
    core_mate = t + 1 - 2 * (t % 2)
    far_mate = (t + 2) % n_tensor
    diagonal = (core_mate + 2) % n_tensor

    def at_seq(i):
        return {"seq": (s + i) % n_seq}

    depth = hidden_ref.shape[1] // UNITED_CHUNKS
    ud_copies = [
        pltpu.make_async_copy(
            ud_hbm.at[:, pl.ds(i * depth, depth)],
            ud_vm.at[:, pl.ds(i * depth, depth)],
            ud_sem.at[i],
        )
        for i in range(UNITED_CHUNKS)
    ]
    for copy in ud_copies:
        copy.start()
    head_cols = pl.ds(pl.multiple_of(s * (own_heads * NOPE), LANES), own_heads * NOPE)
    qu_copy = pltpu.make_async_copy(qu_hbm, qu_vm, w_sem.at[0])
    ku_copy = pltpu.make_async_copy(ku_hbm.at[:, head_cols], ku_vm, w_sem.at[1])
    vu_copy = pltpu.make_async_copy(vu_hbm.at[:, head_cols], vu_vm, w_sem.at[2])
    lat_copy = pltpu.make_async_copy(lat_hbm, lat_vm.at[t], loc_sem.at[0])
    rope_copy = pltpu.make_async_copy(rope_hbm, rope_vm.at[t], loc_sem.at[1])
    for copy in (qu_copy, ku_copy, vu_copy, lat_copy, rope_copy):
        copy.start()

    barrier = pltpu.get_barrier_semaphore()
    for i in range(1, n_seq):
        pl.semaphore_signal(barrier, inc=1, device_id=at_seq(i), device_id_type=MESH_ID)
    for i in range(1, n_tensor):
        pl.semaphore_signal(
            barrier, inc=1, device_id={"tensor": (t + i) % n_tensor}, device_id_type=MESH_ID
        )
    pl.semaphore_wait(barrier, n_seq - 1 + n_tensor - 1)

    def block_copies(src_lat, src_rope, owner, c, send, recv, target):
        at = pl.ds(c * GROUP, GROUP)
        return (
            pltpu.make_async_remote_copy(
                src_ref=src_lat.at[at],
                dst_ref=lat_vm.at[owner, at],
                send_sem=send.at[c, 0],
                recv_sem=recv.at[c, 0],
                device_id={"tensor": target},
                device_id_type=MESH_ID,
            ),
            pltpu.make_async_remote_copy(
                src_ref=src_rope.at[at],
                dst_ref=rope_vm.at[owner, at],
                send_sem=send.at[c, 1],
                recv_sem=recv.at[c, 1],
                device_id={"tensor": target},
                device_id_type=MESH_ID,
            ),
        )

    def y_copies(c):
        return block_copies(lat_hbm, rope_hbm, t, c, y_send, y_recv, far_mate)

    def c_copies(c):
        return block_copies(lat_hbm, rope_hbm, t, c, c_send, c_recv, core_mate)

    def d_copies(c):
        return block_copies(
            lat_vm.at[far_mate], rope_vm.at[far_mate], far_mate, c, d_send, d_recv, core_mate
        )

    total = jnp.zeros((batch, united_cols), jnp.float32)
    for i, copy in enumerate(ud_copies):
        copy.wait()
        total = total + lax.dot_general(
            hidden_ref[:, i * depth : (i + 1) * depth],
            ud_vm[:, i * depth : (i + 1) * depth],
            (((1,), (1,)), ((), ())),
            preferred_element_type=jnp.float32,
        )
    uni_vm[t] = jnp.zeros(uni_vm.shape[1:], jnp.bfloat16)
    uni_vm[t, :, :united_cols] = total.astype(jnp.bfloat16)

    def u_copy(i):
        return pltpu.make_async_remote_copy(
            src_ref=uni_vm.at[t],
            dst_ref=uni_vm.at[t],
            send_sem=u_send.at[i],
            recv_sem=u_recv.at[i],
            device_id={"tensor": (t + i) % n_tensor},
            device_id_type=MESH_ID,
        )

    u_copies = [u_copy(i) for i in range(1, n_tensor)]
    for copy in u_copies:
        copy.start()
    for c in range(groups):
        for copy in y_copies(c):
            copy.start()
    for c in range(groups):
        for copy in c_copies(c):
            copy.start()
    for copy in u_copies:
        copy.wait()
    uw_vm[...] = jnp.zeros(uw_vm.shape, jnp.float32)
    wide_cols = uni_vm.shape[2]
    for i in range(n_tensor):
        base = united_cols * i // LANES * LANES
        shift = united_cols * i - base
        piece = uni_vm[i].astype(jnp.float32)
        if shift:
            piece = pltpu.roll(piece, shift, 1)
        uw_vm[:, base : base + wide_cols] = uw_vm[:, base : base + wide_cols] + piece

    lane_at = lax.broadcasted_iota(jnp.int32, (batch, LANES), 1)
    half = rope_width // 2
    row_at = lax.broadcasted_iota(jnp.int32, (batch, LANES), 0)
    positions = jnp.zeros((batch, LANES), jnp.float32)
    for b in range(batch):
        positions = jnp.where(row_at == b, len_ref[b].astype(jnp.float32), positions)
    freq = jnp.exp((lane_at % half).astype(jnp.float32) * (-2.0 * math.log(10000.0) / rope_width))
    angles = positions * freq
    cos_wide = jnp.where(lane_at < rope_width, jnp.cos(angles), 0.0)
    sine = jnp.sin(angles)
    sin_wide = jnp.where(lane_at < half, -sine, jnp.where(lane_at < rope_width, sine, 0.0))
    latent_part = uw_vm[:, :QR]
    ql_vm[...] = rms_scale(latent_part, q_gain_ref[...].reshape(1, QR)).astype(jnp.bfloat16).astype(jnp.float32)
    new_latent = rms_scale(uw_vm[:, QR : QR + rank], kv_gain_ref[...].reshape(1, rank)).astype(jnp.bfloat16)
    new_rope = rotate_wide(
        uw_vm[:, QR + rank : QR + rank + LANES], cos_wide, sin_wide, lane_at, half
    ).astype(jnp.bfloat16)
    ne_ref[:, :rank] = new_latent
    ne_ref[:, rank:] = new_rope[:, :rope_width]
    nep_vm[:, :rank] = new_latent.astype(jnp.float32)
    nep_vm[:, rank:] = new_rope.astype(jnp.float32)

    row_base = pl.multiple_of(s * rows // LANES * LANES, LANES)
    row_window = ql_vm[:, pl.ds(row_base, 2 * LANES)]
    row_window = jnp.where(
        (s * rows) % LANES == 0, row_window, pltpu.roll(row_window, 2 * LANES - LANES // 2, 1)
    )
    own_query = row_window[:, :rows].astype(jnp.bfloat16)
    qu_copy.wait()
    chunk_cols = own_heads * QH

    def q_copy(i):
        return pltpu.make_async_remote_copy(
            src_ref=qs_vm.at[i],
            dst_ref=qr_vm.at[i],
            send_sem=q_send.at[i],
            recv_sem=q_recv.at[i],
            device_id=at_seq(i),
            device_id_type=MESH_ID,
        )

    for i in list(range(1, n_seq)) + [0]:
        cols = pl.ds(pl.multiple_of((s + i) % n_seq * chunk_cols, LANES), chunk_cols)
        qs_vm[i] = jnp.dot(own_query, qu_vm[:, cols], preferred_element_type=jnp.float32)
        if i:
            q_copy(i).start()
    query = qs_vm[0]
    for i in range(1, n_seq):
        q_copy(i).wait()
        query = query + qr_vm[i]

    score_scale = QH ** (-0.5)
    ku_copy.wait()
    pair = 2 * QH
    for h in range(own_heads):
        both = query[:, h // 2 * pair : (h // 2 + 1) * pair]
        start = 0
        if h % 2:
            both = pltpu.roll(both, pair - LANES // 2, 1)
            start = LANES
        nope = both[:, start : start + NOPE].astype(jnp.bfloat16)
        if h % 2:
            rope = both[:, 2 * LANES : 3 * LANES]
        else:
            rope = both[:, LANES : 2 * LANES]
        absorbed = lax.dot_general(
            nope,
            ku_vm[:, h * NOPE : (h + 1) * NOPE],
            (((1,), (1,)), ((), ())),
            preferred_element_type=jnp.float32,
        )
        at = pl.ds(h * batch, batch)
        pack_vm[0, at, :rank] = (absorbed * score_scale).astype(jnp.bfloat16)
        pack_vm[0, at, rank:] = (
            rotate_wide(rope, cos_wide, sin_wide, lane_at, half) * score_scale
        ).astype(jnp.bfloat16)

    def p_copy(i):
        return pltpu.make_async_remote_copy(
            src_ref=pack_vm.at[0],
            dst_ref=pack_vm.at[i],
            send_sem=p_send.at[i],
            recv_sem=p_recv.at[i],
            device_id=at_seq(i),
            device_id_type=MESH_ID,
        )

    for i in range(1, n_seq):
        p_copy(i).start()
    for i in range(1, n_seq):
        p_copy(i).wait()
    for b0 in range(0, batch, 4):
        part_rows = 4 * heads
        want = lax.broadcasted_iota(jnp.int32, (part_rows, all_rows), 0)
        have = lax.broadcasted_iota(jnp.int32, (part_rows, all_rows), 1)
        want_b = b0 + want // heads
        want_h = want % heads
        slot = (s + n_seq - want_h // own_heads) % n_seq
        source = slot * own_rows + want_h % own_heads * batch + want_b
        hot = jnp.where(have == source, 1.0, 0.0).astype(jnp.bfloat16)
        ordered = jnp.dot(
            hot,
            pack_vm[...].reshape(all_rows, pack_width),
            preferred_element_type=jnp.float32,
        ).astype(jnp.bfloat16)
        qall_vm[b0 : b0 + 4] = ordered.reshape(4, heads, pack_width)

    position = lax.broadcasted_iota(jnp.int32, (heads, BLOCK_POSITIONS), 1)

    def attend_one(owner, k):
        slot = owner * blocks + k
        flat = idx_ref[slot]
        seq_of = flat // span_blocks
        base = (s * span_blocks + flat % span_blocks) * BLOCK_POSITIONS
        limit = len_ref[seq_of] - base
        q = qall_vm[seq_of]
        latent = lat_vm[owner, k]
        scores = lax.dot_general(
            q[:, :rank], latent, (((1,), (1,)), ((), ())), preferred_element_type=jnp.float32
        )
        scores = scores + jnp.dot(
            q[:, rank : rank + rope_width], rope_vm[owner, k], preferred_element_type=jnp.float32
        )
        valid = position < limit
        scores = jnp.where(valid, scores, FLOOR_SCORE)
        top = jnp.max(scores, axis=1, keepdims=True)
        weights = jnp.where(valid, jnp.exp(scores - top), 0.0)
        amount = jnp.sum(weights, axis=1, keepdims=True)
        mixed = jnp.dot(weights.astype(jnp.bfloat16), latent, preferred_element_type=jnp.float32)
        mix_vm[slot] = mixed
        top_vm[slot] = jnp.broadcast_to(top, (heads, LANES))
        tot_vm[slot] = jnp.broadcast_to(amount, (heads, LANES))

    def attend_group(owner, c):
        for k in range(GROUP):
            attend_one(owner, c * GROUP + k)

    lat_copy.wait()
    rope_copy.wait()

    def own_step(c, carry):
        attend_group(t, c)
        return carry

    lax.fori_loop(0, groups, own_step, 0)

    def mate_step(c, carry):
        for copy in c_copies(c):
            copy.wait()
        attend_group(core_mate, c)
        return carry

    lax.fori_loop(0, groups, mate_step, 0)

    def far_step(c, carry):
        for copy in y_copies(c):
            copy.wait()
        for copy in d_copies(c):
            copy.start()
        attend_group(far_mate, c)
        for copy in d_copies(c):
            copy.wait()
        attend_group(diagonal, c)
        return carry

    lax.fori_loop(0, groups, far_step, 0)

    lane_wide = lax.broadcasted_iota(jnp.int32, (heads, LANES), 1)

    def merge_step(b, carry):
        slots = [idx_ref[n_tensor * blocks + b * span_blocks + j] for j in range(span_blocks)]
        tops = [top_vm[slot] for slot in slots]
        top = functools.reduce(jnp.maximum, tops)
        total = jnp.zeros((heads, LANES), jnp.float32)
        mixed = jnp.zeros((heads, rank), jnp.float32)
        for slot, one in zip(slots, tops):
            factor = jnp.exp(one - top)
            total = total + tot_vm[slot] * factor
            mixed = mixed + mix_vm[slot] * factor[:, :1]
        stats = jnp.zeros((heads, LANES), jnp.float32)
        for lane, piece in enumerate(split_three(top) + split_three(total)):
            stats = jnp.where(lane_wide == lane, piece.astype(jnp.float32), stats)
        at = pl.ds(pl.multiple_of(b * heads, heads), heads)
        mixall_vm[at, :rank] = mixed.astype(jnp.bfloat16)
        mixall_vm[at, rank:] = stats.astype(jnp.bfloat16)
        return carry

    lax.fori_loop(0, batch, merge_step, 0)

    def m_copy(i):
        return pltpu.make_async_remote_copy(
            src_ref=part_vm.at[i],
            dst_ref=got_vm.at[i],
            send_sem=m_send.at[i],
            recv_sem=m_recv.at[i],
            device_id=at_seq(i),
            device_id_type=MESH_ID,
        )

    want = lax.broadcasted_iota(jnp.int32, (own_rows, all_rows), 0)
    have = lax.broadcasted_iota(jnp.int32, (own_rows, all_rows), 1)
    local_source = want % batch * heads + want // batch
    for i in list(range(1, n_seq)) + [0]:
        peer = (s + i) % n_seq
        hot = jnp.where(have == local_source + peer * own_heads, 1.0, 0.0).astype(jnp.bfloat16)
        chosen = jnp.dot(hot, mixall_vm[...], preferred_element_type=jnp.float32).astype(
            jnp.bfloat16
        )
        if i:
            part_vm[i] = chosen
            m_copy(i).start()
        else:
            got_vm[0] = chosen

    pack = pack_vm[0].astype(jnp.float32)
    entry = jnp.concatenate([nep_vm[...]] * own_heads, axis=0)
    own_score = jnp.sum(pack * entry, axis=1, keepdims=True)
    for i in range(1, n_seq):
        m_copy(i).wait()
    tops = []
    totals = []
    for i in range(n_seq):
        stats = got_vm[i, :, rank:].astype(jnp.float32)
        tops.append(stats[:, 0:1] + stats[:, 1:2] + stats[:, 2:3])
        totals.append(stats[:, 3:4] + stats[:, 4:5] + stats[:, 5:6])
    final_top = functools.reduce(jnp.maximum, tops, own_score)
    own_weight = jnp.exp(own_score - final_top)
    total = own_weight
    mixture = own_weight.astype(jnp.bfloat16).astype(jnp.float32) * entry[:, :rank]
    for i in range(n_seq):
        factor = jnp.exp(tops[i] - final_top)
        total = total + totals[i] * factor
        mixture = mixture + got_vm[i, :, :rank].astype(jnp.float32) * factor
    attended = (mixture / total).astype(jnp.bfloat16)
    vu_copy.wait()
    for h in range(own_heads):
        out_vm[0, :, h * VD : (h + 1) * VD] = jnp.dot(
            attended[h * batch : (h + 1) * batch],
            vu_vm[:, h * VD : (h + 1) * VD],
            preferred_element_type=jnp.float32,
        ).astype(jnp.bfloat16)

    def o_copy(i):
        return pltpu.make_async_remote_copy(
            src_ref=out_vm.at[0],
            dst_ref=out_vm.at[i],
            send_sem=o_send.at[i],
            recv_sem=o_recv.at[i],
            device_id=at_seq(i),
            device_id_type=MESH_ID,
        )

    for i in range(1, n_seq):
        o_copy(i).start()
    for i in range(n_seq):
        if i:
            o_copy(i).wait()
        cols = pl.ds(
            pl.multiple_of((s + n_seq - i) % n_seq * (own_heads * VD), LANES), own_heads * VD
        )
        out_ref[:, cols] = out_vm[i]


def kernel_body(
    n_seq,
    n_tensor,
    hidden_in,
    united_down,
    q_gain,
    kv_gain,
    q_up,
    key_up,
    value_up,
    latent_block_store,
    rope_pool,
    lengths,
    block_table,
):
    batch, width = hidden_in.shape
    heads = key_up.shape[1] // NOPE
    own_heads = heads // n_seq
    span_blocks = block_table.shape[1]
    blocks = latent_block_store.shape[0]
    rope_width = rope_pool.shape[1]
    united_cols = united_down.shape[1]
    seq_index = lax.axis_index("seq")
    local_table = block_table.reshape(-1) - seq_index * (batch * span_blocks)
    flat_index = jnp.arange(local_table.shape[0], dtype=jnp.int32)
    slot_at = jnp.arange(n_tensor * blocks, dtype=jnp.int32)
    owner = jnp.sum(
        jnp.where(local_table[None, :] == slot_at[:, None], flat_index[None, :], 0), axis=1
    )
    places = jnp.concatenate([owner, local_table])
    dims = dict(
        heads=heads,
        own_heads=own_heads,
        batch=batch,
        span_blocks=span_blocks,
        blocks=blocks,
        united_cols=united_cols,
        rope_width=rope_width,
        rows=q_up.shape[0],
    )
    wide_cols = -(-united_cols // LANES) * LANES
    united_all = -(-united_cols * n_tensor // LANES) * LANES + 4 * LANES
    pack_width = LATENT_RANK + LANES
    own_rows = own_heads * batch
    all_rows = heads * batch
    groups = blocks // GROUP
    slots = n_tensor * blocks
    vmem = pl.BlockSpec(memory_space=pltpu.VMEM)
    smem = pl.BlockSpec(memory_space=pltpu.SMEM)
    anywhere = pl.BlockSpec(memory_space=pl.ANY)
    dma = pltpu.SemaphoreType.DMA
    bf16, f32 = jnp.bfloat16, jnp.float32
    out, new_entry = pl.pallas_call(
        functools.partial(step_kernel, n_seq, n_tensor, dims),
        out_shape=(
            jax.ShapeDtypeStruct((batch, heads * VD), bf16),
            jax.ShapeDtypeStruct((batch, LATENT_RANK + rope_width), bf16),
        ),
        in_specs=[smem, smem] + [vmem] * 3 + [anywhere] * 6,
        out_specs=(vmem, vmem),
        scratch_shapes=[
            pltpu.VMEM(united_down.shape[::-1], bf16),
            pltpu.VMEM(q_up.shape, bf16),
            pltpu.VMEM((LATENT_RANK, own_heads * NOPE), bf16),
            pltpu.VMEM((LATENT_RANK, own_heads * VD), bf16),
            pltpu.VMEM((n_tensor,) + latent_block_store.shape, bf16),
            pltpu.VMEM((n_tensor,) + rope_pool.shape, bf16),
            pltpu.VMEM((n_tensor, batch, wide_cols), bf16),
            pltpu.VMEM((batch, united_all), f32),
            pltpu.VMEM((batch, QR), f32),
            pltpu.VMEM((batch, pack_width), f32),
            pltpu.VMEM((n_seq, batch, own_heads * QH), f32),
            pltpu.VMEM((n_seq, batch, own_heads * QH), f32),
            pltpu.VMEM((n_seq, own_rows, pack_width), bf16),
            pltpu.VMEM((batch, heads, pack_width), bf16),
            pltpu.VMEM((slots, heads, LATENT_RANK), f32),
            pltpu.VMEM((slots, heads, LANES), f32),
            pltpu.VMEM((slots, heads, LANES), f32),
            pltpu.VMEM((all_rows, pack_width), bf16),
            pltpu.VMEM((n_seq, own_rows, pack_width), bf16),
            pltpu.VMEM((n_seq, own_rows, pack_width), bf16),
            pltpu.VMEM((n_seq, batch, own_heads * VD), bf16),
            dma((UNITED_CHUNKS,)),
            dma((3,)),
            dma((2,)),
            dma((n_tensor,)),
            dma((n_tensor,)),
            dma((groups, 2)),
            dma((groups, 2)),
            dma((groups, 2)),
            dma((groups, 2)),
            dma((groups, 2)),
            dma((groups, 2)),
        ]
        + [dma((n_seq,))] * 8,
        compiler_params=pltpu.CompilerParams(
            collective_id=0, has_side_effects=True, vmem_limit_bytes=60 * 1024 * 1024
        ),
    )(
        places,
        lengths,
        hidden_in,
        q_gain,
        kv_gain,
        united_down.T,
        q_up,
        key_up,
        value_up,
        latent_block_store,
        rope_pool,
    )
    return (out, new_entry)


def body_for(n_seq, n_tensor):
    def body(*args):
        q_up, key_up, latents = args[4], args[5], args[7]
        heads = key_up.shape[1] // NOPE
        fits = n_tensor == 4 and heads % (2 * n_seq) == 0 and latents.shape[0] % GROUP == 0
        fits = fits and q_up.shape[0] % (LANES // 2) == 0 and q_up.shape[0] <= LANES + LANES // 2
        if fits:
            return kernel_body(n_seq, n_tensor, *args)
        return plain_body(*args)

    return body


def solution(mesh):
    in_specs = (
        P(),
        P(None, "tensor"),
        P(),
        P(),
        P("seq", "tensor"),
        P(None, "tensor"),
        P(None, "tensor"),
        P(("seq", "tensor"), None, None),
        P(("seq", "tensor"), None, None),
        P(),
        P(None, "seq"),
    )
    out_specs = (P(None, "tensor"), P())
    return jax.shard_map(
        body_for(mesh.shape["seq"], mesh.shape["tensor"]), mesh=mesh, in_specs=in_specs, out_specs=out_specs, check_vma=False)
```
